32 devices in a mesh: rows: 8 (over z, x), cols: 4 (over y, core).
Axes of the slice: x: 2, y: 2, z: 4, core: 2. Of those that a mesh axis runs over, the one named last changes fastest.
Arguments:
- densities: bfloat16 [6, 2048, 128, 128], P(None, ('rows', 'cols')), may hold values from -6 to 6
- residuals: bfloat16 [6, 2048, 128, 128], P(None, ('rows', 'cols')), may hold values from -32 to 32
- block_pairs: int32 [2, 2048], P(None, ('rows', 'cols')), may hold values from 0 to 1562
- new_owner: int32 [2048], P(('rows', 'cols')), may hold values from -1 to 7, as said below
Outputs:
- owned_blocks: bfloat16 [1024, 128, 128], P(('rows', 'cols'))
- coefficients: float32 [6], replicated
The draws below stay inside these ranges and needn't reach their ends.
Inputs may be any that keep to these rules, and one draw needn't show every extreme that they name: A live block stays at its index of cols and moves to index new_owner of rows. For each index of cols, every index of rows becomes the owner of exactly 32 blocks, and at most 8 of them come from one device.
All inputs are finite; a program needn't handle non-finite values.
Results may differ from the reference program's by a relative error of at most 0.0019.
Values may be sent and summed in bfloat16 or wider, within the bound.
No kernel may reach another device: no remote copies, remote signals or barrier semaphores. Data moves between devices by JAX's collectives and lax.ppermute only.
A program may use at most 128 MiB of HBM per device.

```python
import jax
import jax.numpy as jnp
from jax import lax

BLOCK = 128
ROW_BLOCKS = 1563
HISTORY = 5
OWNED = 32
HELD = 64
SLOTS = 2048
N_ROWS = 8
N_COLS = 4


def draw_residuals(key, part):
    full_shape = (HISTORY + 1, SLOTS, BLOCK, BLOCK)
    key_noise = jax.random.fold_in(key, 0)
    key_scale = jax.random.fold_in(key, 1)
    key_history = jax.random.fold_in(key, 4)
    key_lines = jax.random.fold_in(key, 5)
    key_across = jax.random.fold_in(key, 6)
    device_of = jnp.arange(SLOTS, dtype=jnp.int32) // HELD
    device_count = SLOTS // HELD
    ramp_scale = 1.0 + device_of.astype(jnp.float32) / max(device_count - 1, 1)
    history_scale = jnp.exp(jax.random.uniform(key_history, (HISTORY + 1, SLOTS), jnp.float32, jnp.log(0.35), jnp.log(2.8)))
    line_factor = jnp.exp(jax.random.uniform(key_lines, (HISTORY + 1, 1, BLOCK, 1), jnp.float32, jnp.log(0.1), jnp.log(10.0)))
    across_factor = jnp.exp(jax.random.uniform(key_across, (HISTORY + 1, 1, 1, BLOCK), jnp.float32, jnp.log(0.1), jnp.log(10.0)))
    values = jax.random.normal(key_noise, full_shape, jnp.float32)
    slot_scale = jnp.exp(jax.random.uniform(key_scale, (SLOTS,), jnp.float32, jnp.log(0.25), jnp.log(4.0)))
    values = values * (history_scale * (ramp_scale * slot_scale)[None, :])[:, :, None, None]
    values = 0.06 * values * line_factor * across_factor
    return jnp.clip(values, -32.0, 32.0).astype(jnp.bfloat16)


def draw_block_pairs(key, part):
    key_row, key_col, key_diag = jax.random.split(key, 3)
    row_ids = jax.random.randint(key_row, (SLOTS,), 0, ROW_BLOCKS, dtype=jnp.int32)
    col_ids = jax.random.randint(key_col, (SLOTS,), 0, ROW_BLOCKS, dtype=jnp.int32)
    diagonal = jax.random.randint(key_diag, (SLOTS,), 0, 2, dtype=jnp.int32) == 0
    return jnp.stack([row_ids, jnp.where(diagonal, row_ids, col_ids)]).astype(jnp.int32)


def draw_new_owner(key, part):
    rows_total = N_ROWS
    cols_total = SLOTS // HELD // N_ROWS
    pair_cap = HELD // rows_total
    key_pick, key_perm = jax.random.split(key, 2)
    picks = jax.random.randint(key_pick, (cols_total, rows_total // 4, rows_total), 1, 4, dtype=jnp.int32)
    row_ids = jnp.arange(rows_total, dtype=jnp.int32)
    picked_row = picks[:, row_ids // 4, :]
    sends = (row_ids % 4 == 0)[None, :, None] | ((row_ids % 4)[None, :, None] == picked_row)
    entry_ids = jnp.arange(HELD, dtype=jnp.int32)
    entry_owner = entry_ids // pair_cap
    values = jnp.where(sends[:, :, entry_owner], entry_owner[None, None, :], -1).astype(jnp.int32)
    scores = jax.random.randint(key_perm, (cols_total, rows_total, HELD), 0, 1 << 20, dtype=jnp.int32) * HELD + entry_ids
    orders = jnp.argsort(scores, axis=2, stable=True).astype(jnp.int32)
    column_ids = jnp.arange(cols_total, dtype=jnp.int32)[:, None, None]
    device_ids = row_ids[None, :, None] * cols_total + column_ids
    flat_slot = device_ids * HELD + orders
    return jnp.full((SLOTS,), -1, jnp.int32).at[flat_slot.reshape(-1)].set(values.reshape(-1))


def block_scale(stream_key, shape, shards, smallest, high):
    gain = 1.0
    for dim, blocks in shards:
        steps = jax.random.uniform(jax.random.fold_in(jax.random.fold_in(stream_key, 6), dim), (blocks,), jnp.float32, smallest / len(shards), high / len(shards))
        gain = gain * jnp.repeat(jnp.exp(steps), shape[dim] // blocks).reshape((-1,) + (1,) * (len(shape) - 1 - dim))
    return gain


def scatter_about(own_key, shape, spread, most, cuts=(), kind=jnp.bfloat16):
    level = block_scale(own_key, shape, cuts, -0.22, 0.18) if cuts else 1.0
    values = jax.random.normal(own_key, shape, jnp.float32) * spread * level
    return jnp.minimum(jnp.maximum(values, -most), most).astype(kind)


def setup_inputs(seed: int = 0) -> dict:
    key_list = jax.random.split(jax.random.key(seed), 5)
    densities = scatter_about(key_list[0], (HISTORY + 1, SLOTS, BLOCK, BLOCK), 1.0, 6.0, ((1, 32),))
    residuals = draw_residuals(jax.random.fold_in(key_list[4], 71), 0)
    block_pairs = draw_block_pairs(jax.random.fold_in(key_list[4], 71), 0)
    new_owner = draw_new_owner(jax.random.fold_in(key_list[4], 71), 0)
    return dict(densities=densities, residuals=residuals, block_pairs=block_pairs, new_owner=new_owner)


mix_weight = 0.3


def small_solve(system, vector):
    order_n = system.shape[0]
    positions = jnp.arange(order_n, dtype=jnp.int32)
    for step_index in range(order_n):
        column = system[:, step_index] / system[step_index, step_index]
        column = jnp.where(positions > step_index, column, 0.0)
        system = system - column[:, None] * system[step_index][None, :]
        vector = vector - column * vector[step_index]
    solution = jnp.zeros((order_n,), jnp.float32)
    for step_index in reversed(range(order_n)):
        inner = jnp.sum(jnp.where(positions > step_index, system[step_index] * solution, 0.0))
        solution = solution.at[step_index].set((vector[step_index] - inner) / system[step_index, step_index])
    return solution


def reference(densities, residuals, block_pairs, new_owner):
    slot_total = new_owner.shape[0]
    history_count = densities.shape[0]
    devices_all = N_ROWS * N_COLS
    alive_slot = new_owner >= 0
    slot_weight = jnp.where(alive_slot, jnp.where(block_pairs[0] == block_pairs[1], 1.0, 2.0), 0.0).astype(jnp.float32)

    def gram_step(running, device):
        first_slot = (device * HELD).astype(jnp.int32)
        residual_part = lax.dynamic_slice_in_dim(residuals, first_slot, HELD, 1).astype(jnp.float32)
        weight_part = lax.dynamic_slice_in_dim(slot_weight, first_slot, HELD, 0)
        per_slot = jnp.einsum("isxy,ksxy->sik", residual_part, residual_part, precision=lax.Precision.HIGHEST)
        return running + jnp.einsum("s,sik->ik", weight_part, per_slot, precision=lax.Precision.HIGHEST), None

    correlation = lax.scan(gram_step, jnp.zeros((history_count, history_count), jnp.float32), jnp.arange(devices_all, dtype=jnp.int32))[0]
    solved = small_solve(correlation, jnp.ones((history_count,), jnp.float32))
    coefficients = solved / jnp.sum(solved)

    def blend_step(device):
        first_slot = (device * HELD).astype(jnp.int32)
        density_part = lax.dynamic_slice_in_dim(densities, first_slot, HELD, 1)
        residual_part = lax.dynamic_slice_in_dim(residuals, first_slot, HELD, 1)
        running = jnp.zeros(density_part.shape[1:], jnp.float32)
        for hist_index in range(history_count):
            running = running + coefficients[hist_index] * (density_part[hist_index].astype(jnp.float32) + mix_weight * residual_part[hist_index].astype(jnp.float32))
        return running.astype(jnp.bfloat16)

    mixed_blocks = lax.map(blend_step, jnp.arange(devices_all, dtype=jnp.int32)).reshape(slot_total, BLOCK, BLOCK)
    slot_ids = jnp.arange(slot_total, dtype=jnp.int32)
    column_of = (slot_ids // HELD) % N_COLS
    destination = jnp.where(alive_slot, new_owner * N_COLS + column_of, devices_all).astype(jnp.int32)
    onehot = (destination[:, None] == jnp.arange(devices_all, dtype=jnp.int32)[None, :]).astype(jnp.int32)
    ranking = jnp.sum(jnp.cumsum(onehot, axis=0) * onehot, axis=1) - 1
    target_slot = jnp.where(alive_slot, destination * OWNED + ranking, devices_all * OWNED).astype(jnp.int32)
    owned_blocks = jnp.zeros((devices_all * OWNED, BLOCK, BLOCK), jnp.bfloat16).at[target_slot].set(mixed_blocks, mode="drop")
    return owned_blocks, coefficients
```

```python
import functools

import jax
import jax.numpy as jnp
from jax import lax
from jax.experimental import pallas as pl
from jax.experimental.pallas import tpu as pltpu
from jax.sharding import PartitionSpec as P


OWNED = 32
LANES = 128
SUBLANES = 8
GRAM_SLOTS = 4
MIB = 1024 * 1024

mix_weight = 0.3


def pair_list(order_n):
    return [(i, k) for i in range(order_n) for k in range(i, order_n)]


def partner(index, step, count):
    return index ^ step if count & (count - 1) == 0 else lax.rem(index + step, count)


def pattern_of(owner, index, count):
    return owner ^ index if count & (count - 1) == 0 else lax.rem(owner + count - index, count)


def gram_kernel(rows_count, pair_cap, owner_ref, pairs_ref, residuals_ref, tile_ref, table_ref,
                held_ref, total_ref, weight_ref, count_ref, sems):
    order_n, held_slots = residuals_ref.shape[:2]
    chunks = held_slots // GRAM_SLOTS
    pairs = pair_list(order_n)
    my_row = lax.axis_index("rows")

    def chunk_copy(chunk):
        span = pl.ds(chunk * GRAM_SLOTS, GRAM_SLOTS)
        return pltpu.make_async_copy(residuals_ref.at[:, span], held_ref.at[:, span], sems.at[chunk])

    for chunk in range(chunks):
        chunk_copy(chunk).start()

    for row in range(rows_count):
        count_ref[row] = 0

    def clear(place, carry):
        table_ref[place] = 0
        return carry

    lax.fori_loop(0, rows_count * pair_cap, clear, 0, unroll=8)

    def route(slot, carry):
        owner = owner_ref[slot]
        alive = owner >= 0
        diagonal = pairs_ref[0, slot] == pairs_ref[1, slot]
        weight_ref[slot] = jnp.where(alive, jnp.where(diagonal, 1.0, 2.0), 0.0).astype(jnp.float32)

        @pl.when(alive)
        def _():
            rank = count_ref[owner]
            table_ref[pattern_of(owner, my_row, rows_count) * pair_cap + rank] = slot
            count_ref[owner] = rank + 1

        return carry

    lax.fori_loop(0, held_slots, route, 0, unroll=2)

    total_ref[...] = jnp.zeros_like(total_ref)
    groups = residuals_ref.shape[2] // (2 * SUBLANES)

    def slot_step(slot, carry):
        sums = [None] * len(pairs)
        for group in range(groups):
            rows = pl.ds(group * 2 * SUBLANES, 2 * SUBLANES)
            wide = [held_ref[i, slot, rows, :].astype(jnp.float32) for i in range(order_n)]
            for half in range(2):
                part = [x[half * SUBLANES:(half + 1) * SUBLANES] for x in wide]
                for e, (i, k) in enumerate(pairs):
                    product = part[i] * part[k]
                    sums[e] = product if sums[e] is None else sums[e] + product
        weight = weight_ref[slot]
        for e in range(len(pairs)):
            total_ref[e] += weight * sums[e]
        return carry

    for chunk in range(chunks):
        chunk_copy(chunk).wait()
        lax.fori_loop(chunk * GRAM_SLOTS, (chunk + 1) * GRAM_SLOTS, slot_step, 0)

    lanes = lax.broadcasted_iota(jnp.int32, (1, LANES), 1)
    entry_row = jnp.zeros((1, LANES), jnp.float32)
    for e in range(len(pairs)):
        entry = jnp.sum(jnp.sum(total_ref[e], axis=0, keepdims=True), axis=1, keepdims=True)
        entry_row = jnp.where(lanes == e, entry, entry_row)
    count_row = jnp.zeros((1, LANES), jnp.float32)
    for row in range(rows_count):
        count_row = jnp.where(lanes == row, count_ref[row].astype(jnp.float32), count_row)
    rows = lax.broadcasted_iota(jnp.int32, (SUBLANES, LANES), 0)
    tile = jnp.where(rows == 0, entry_row, jnp.where(rows == 1, count_row, 0.0))
    tile_ref[...] = jnp.broadcast_to(tile[None], tile_ref.shape)


def gram_call(residuals, block_pairs, new_owner, rows_count, device_count, pair_cap):
    order_n, held_slots = residuals.shape[:2]
    return pl.pallas_call(
        functools.partial(gram_kernel, rows_count, pair_cap),
        out_shape=(
            jax.ShapeDtypeStruct((device_count, SUBLANES, LANES), jnp.float32),
            jax.ShapeDtypeStruct((rows_count * pair_cap,), jnp.int32),
        ),
        in_specs=[
            pl.BlockSpec(memory_space=pltpu.SMEM),
            pl.BlockSpec(memory_space=pltpu.SMEM),
            pl.BlockSpec(memory_space=pltpu.HBM),
        ],
        out_specs=(
            pl.BlockSpec(memory_space=pltpu.VMEM),
            pl.BlockSpec(memory_space=pltpu.SMEM),
        ),
        scratch_shapes=[
            pltpu.VMEM(residuals.shape, residuals.dtype),
            pltpu.VMEM((len(pair_list(order_n)), SUBLANES, LANES), jnp.float32),
            pltpu.SMEM((held_slots,), jnp.float32),
            pltpu.SMEM((rows_count,), jnp.int32),
            pltpu.SemaphoreType.DMA((held_slots // GRAM_SLOTS,)),
        ],
        compiler_params=pltpu.CompilerParams(vmem_limit_bytes=20 * MIB),
        name="gram",
    )(new_owner, block_pairs, residuals)


def solve_rows(total, order_n):
    entry = {}
    for e, (i, k) in enumerate(pair_list(order_n)):
        entry[i, k] = jnp.broadcast_to(total[0:1, e:e + 1], (SUBLANES, LANES))
    vector = [jnp.ones((SUBLANES, LANES), jnp.float32)] * order_n
    for step in range(order_n):
        for i in range(step + 1, order_n):
            factor = entry[step, i] / entry[step, step]
            for k in range(i, order_n):
                entry[i, k] = entry[i, k] - factor * entry[step, k]
            vector[i] = vector[i] - factor * vector[step]
    solved = [None] * order_n
    for step in reversed(range(order_n)):
        inner = vector[step]
        for k in range(step + 1, order_n):
            inner = inner - entry[step, k] * solved[k]
        solved[step] = inner / entry[step, step]
    whole = functools.reduce(jnp.add, solved)
    return [x / whole for x in solved]


def blend_kernel(solving, step, pair_cap, table_ref, head_ref, densities_ref, residuals_ref, *rest):
    if solving:
        mixed_ref, coef_ref, density_ref, residual_ref, sems = rest
    else:
        mixed_ref, density_ref, residual_ref, sems = rest
    order_n = densities_ref.shape[0]

    def copies(place):
        slot = table_ref[step * pair_cap + place]
        return (
            pltpu.make_async_copy(densities_ref.at[:, slot], density_ref.at[:, place], sems.at[0, place]),
            pltpu.make_async_copy(residuals_ref.at[:, slot], residual_ref.at[:, place], sems.at[1, place]),
        )

    for place in range(pair_cap):
        for copy in copies(place):
            copy.start()
    if solving:
        coefs = solve_rows(jnp.sum(head_ref[...], axis=0), order_n)
        rows = lax.broadcasted_iota(jnp.int32, (SUBLANES, LANES), 0)
        stacked = jnp.zeros((SUBLANES, LANES), jnp.float32)
        for i in range(order_n):
            stacked = jnp.where(rows == i, coefs[i], stacked)
        coef_ref[...] = stacked
    else:
        coefs = [jnp.broadcast_to(head_ref[i:i + 1, :], (SUBLANES, LANES)) for i in range(order_n)]
    coefs = [jnp.concatenate([c, c], axis=0) for c in coefs]
    groups = mixed_ref.shape[1] // (2 * SUBLANES)
    for place in range(pair_cap):
        for copy in copies(place):
            copy.wait()
        for group in range(groups):
            rows = pl.ds(group * 2 * SUBLANES, 2 * SUBLANES)
            running = None
            for i in range(order_n):
                term = coefs[i] * (
                    density_ref[i, place, rows, :].astype(jnp.float32)
                    + mix_weight * residual_ref[i, place, rows, :].astype(jnp.float32)
                )
                running = term if running is None else running + term
            mixed_ref[place, rows, :] = running.astype(mixed_ref.dtype)


def blend_call(solving, step, pair_cap, table, head, densities, residuals):
    order_n = densities.shape[0]
    block = densities.shape[2:]
    mixed = pltpu.VMEM((pair_cap,) + block, jnp.bfloat16)
    coef = jax.ShapeDtypeStruct((SUBLANES, LANES), jnp.float32)
    vmem = pl.BlockSpec(memory_space=pltpu.VMEM)
    return pl.pallas_call(
        functools.partial(blend_kernel, solving, step, pair_cap),
        out_shape=(mixed, coef) if solving else mixed,
        in_specs=[
            pl.BlockSpec(memory_space=pltpu.SMEM),
            vmem,
            pl.BlockSpec(memory_space=pltpu.HBM),
            pl.BlockSpec(memory_space=pltpu.HBM),
        ],
        out_specs=(vmem, vmem) if solving else vmem,
        scratch_shapes=[
            pltpu.VMEM((order_n, pair_cap) + block, densities.dtype),
            pltpu.VMEM((order_n, pair_cap) + block, residuals.dtype),
            pltpu.SemaphoreType.DMA((2, pair_cap)),
        ],
        compiler_params=pltpu.CompilerParams(vmem_limit_bytes=8 * MIB),
    )(table, head, densities, residuals)


def place_kernel(rows_count, pair_cap, count_ref, offset_ref, *rest):
    arrived = rest[:rows_count]
    owned_ref, sem = rest[rows_count:]

    def each(act):
        for step in range(rows_count):
            for place in range(pair_cap):

                @pl.when(place < count_ref[step])
                def _():
                    act(pltpu.make_async_copy(
                        arrived[step].at[place],
                        owned_ref.at[offset_ref[step] + place],
                        sem.at[step, place],
                    ))

    each(lambda copy: copy.start())
    each(lambda copy: copy.wait())


def place_call(counts, offsets, arrived):
    rows_count, pair_cap = len(arrived), arrived[0].shape[0]
    smem = pl.BlockSpec(memory_space=pltpu.SMEM)
    return pl.pallas_call(
        functools.partial(place_kernel, rows_count, pair_cap),
        out_shape=jax.ShapeDtypeStruct((OWNED,) + arrived[0].shape[1:], arrived[0].dtype),
        in_specs=[smem, smem] + [pl.BlockSpec(memory_space=pltpu.VMEM)] * rows_count,
        out_specs=pl.BlockSpec(memory_space=pl.ANY),
        scratch_shapes=[pltpu.SemaphoreType.DMA((rows_count, pair_cap))],
        compiler_params=pltpu.CompilerParams(vmem_limit_bytes=8 * MIB),
        name="place",
    )(counts, offsets, *[pltpu.with_memory_space_constraint(x, pltpu.VMEM) for x in arrived])


def step_order(rows_count):
    return [*range(rows_count // 2, rows_count), *range(1, rows_count // 2), 0]


def on_device(densities, residuals, block_pairs, new_owner):
    rows_count = lax.axis_size("rows")
    cols_count = lax.axis_size("cols")
    order_n = densities.shape[0]
    densities = pltpu.with_memory_space_constraint(densities, pltpu.HBM)
    residuals = pltpu.with_memory_space_constraint(residuals, pltpu.HBM)
    pair_cap = 2 * OWNED // rows_count
    my_row, my_col = lax.axis_index("rows"), lax.axis_index("cols")
    tiles, table = gram_call(
        residuals, block_pairs, new_owner, rows_count, rows_count * cols_count, pair_cap
    )
    tiles = lax.all_to_all(tiles, ("rows", "cols"), split_axis=0, concat_axis=0, tiled=True)

    arrived = [None] * rows_count
    head = pltpu.with_memory_space_constraint(tiles, pltpu.VMEM)
    coef = None
    for step in step_order(rows_count):
        if coef is None:
            mixed, coef = blend_call(True, step, pair_cap, table, head, densities, residuals)
        else:
            mixed = blend_call(False, step, pair_cap, table, coef, densities, residuals)
        if step:
            pairs = [(row, int(partner(row, step, rows_count))) for row in range(rows_count)]
            mixed = lax.ppermute(mixed, "rows", pairs)
        arrived[step] = mixed

    by_row = tiles.reshape(rows_count, cols_count, SUBLANES, LANES)[:, :, 1, :]
    by_row = lax.dynamic_index_in_dim(by_row, my_col, 1, keepdims=False)
    by_row = lax.dynamic_index_in_dim(by_row, my_row, 1, keepdims=False)
    row_ids = jnp.arange(rows_count, dtype=jnp.int32)
    from_row = row_ids ^ my_row if rows_count & (rows_count - 1) == 0 else (
        row_ids * -1 + my_row + rows_count) % rows_count
    counts = jnp.sum(jnp.where(from_row[:, None] == row_ids[None, :], by_row[None, :], 0.0), axis=1)
    offsets = jnp.sum(jnp.where(from_row[:, None] > row_ids[None, :], by_row[None, :], 0.0), axis=1)
    owned_blocks = place_call(counts.astype(jnp.int32), offsets.astype(jnp.int32), arrived)
    return (owned_blocks, coef[:order_n, 0])


def solution(mesh):
    return jax.shard_map(
        on_device,
        mesh=mesh,
        in_specs=(
            P(None, ("rows", "cols"), None, None),
            P(None, ("rows", "cols"), None, None),
            P(None, ("rows", "cols")),
            P(("rows", "cols")),
        ),
        out_specs=(P(("rows", "cols"), None, None), P()),
        check_vma=False,
    )
```

```python
import functools

import jax
import jax.numpy as jnp
from jax import lax
from jax.experimental import pallas as pl
from jax.experimental.pallas import tpu as pltpu
from jax.sharding import PartitionSpec as P


OWNED = 32
LANES = 128
SUBLANES = 8
GRAM_SLOTS = 16
ROUTING = 2
TILE = 4
COUNT_LANE = 64
MIB = 1024 * 1024

mix_weight = 0.3


def pair_list(order_n):
    return [(i, k) for i in range(order_n) for k in range(i, order_n)]


def partner(index, step, count):
    return index ^ step if count & (count - 1) == 0 else lax.rem(index + step, count)


def pattern_of(owner, index, count):
    return owner ^ index if count & (count - 1) == 0 else lax.rem(owner + count - index, count)


def gram_kernel(rows_count, pair_cap, owner_hbm, pairs_hbm, residuals_ref, tile_ref, table_ref,
                held_ref, low_ref, high_ref, owner_ref, pairs_ref, count_ref, sems, index_sems):
    order_n, held_slots = residuals_ref.shape[:2]
    chunks = held_slots // GRAM_SLOTS
    pairs = pair_list(order_n)
    my_row = lax.axis_index("rows")
    sent_count = rows_count * pair_cap

    def chunk_copy(chunk):
        span = pl.ds(chunk * GRAM_SLOTS, GRAM_SLOTS)
        return pltpu.make_async_copy(residuals_ref.at[:, span], held_ref.at[:, span], sems.at[chunk])

    index_copies = (
        pltpu.make_async_copy(owner_hbm, owner_ref, index_sems.at[0]),
        pltpu.make_async_copy(pairs_hbm, pairs_ref, index_sems.at[1]),
    )
    for copy in index_copies:
        copy.start()
    for chunk in range(chunks):
        chunk_copy(chunk).start()

    for row in range(rows_count + 1):
        count_ref[row] = 0

    def clear(place, carry):
        table_ref[place] = 0
        return carry

    lax.fori_loop(0, sent_count, clear, 0, unroll=8)
    for ref in (low_ref, high_ref):
        ref[...] = jnp.zeros_like(ref)
    for copy in index_copies:
        copy.wait()

    def route(slot):
        owner = owner_ref[slot]
        alive = owner >= 0
        bucket = jnp.where(alive, owner, rows_count)
        rank = count_ref[bucket]
        count_ref[bucket] = rank + 1
        place = pattern_of(owner, my_row, rows_count) * pair_cap + rank
        table_ref[jnp.where(alive, place, sent_count)] = slot

    block_rows = residuals_ref.shape[2]
    half_rows = block_rows // 2

    def weight_of(slot):
        alive = owner_ref[slot] >= 0
        diagonal = pairs_ref[0, slot] == pairs_ref[1, slot]
        return jnp.where(alive, jnp.where(diagonal, 1.0, 2.0), 0.0).astype(jnp.float32)

    def matrix_slots(slots):
        plain = [
            jnp.concatenate(
                [held_ref[i, slot, pl.ds(start, half_rows), :] for slot in slots for start in (0, half_rows)],
                axis=1,
            )
            for i in range(order_n)
        ]
        weight = jnp.concatenate(
            [jnp.full((half_rows, 2 * LANES), weight_of(slot), jnp.float32).astype(jnp.bfloat16) for slot in slots],
            axis=1,
        )
        scaled = [x * weight for x in plain]
        for ref, span in ((low_ref, range(TILE)), (high_ref, range(TILE, order_n))):
            ref[...] += lax.dot_general(
                jnp.concatenate(scaled[span[0]:], axis=0),
                jnp.concatenate([plain[i] for i in span], axis=0),
                (((1,), (1,)), ((), ())),
                preferred_element_type=jnp.float32,
            )

    def chunk_step(routed, chunk, carry):
        chunk_copy(chunk).wait()
        for i in range(routed):
            route(chunk * routed + i)
        first_slot = chunk * GRAM_SLOTS
        matrix_slots([first_slot + i for i in range(GRAM_SLOTS)])
        return carry

    routing_chunks = chunks // ROUTING
    lax.fori_loop(0, routing_chunks, functools.partial(chunk_step, held_slots // routing_chunks), 0)
    lax.fori_loop(routing_chunks, chunks, functools.partial(chunk_step, 0), 0)

    lanes = lax.broadcasted_iota(jnp.int32, (1, LANES), 1)
    row = jnp.zeros((1, LANES), jnp.float32)
    for owner in range(rows_count):
        row = jnp.where(lanes == COUNT_LANE + owner, count_ref[owner].astype(jnp.float32), row)
    diagonals = {}
    for ref, span in ((low_ref, range(TILE)), (high_ref, range(TILE, order_n))):
        width = ref.shape[1]
        across = lax.broadcasted_iota(jnp.int32, (half_rows, width), 1)
        down = lax.broadcasted_iota(jnp.int32, (half_rows, width), 0)
        on_diagonal = across % half_rows == down
        for k in range(span[0], order_n):
            block = ref[pl.ds((k - span[0]) * half_rows, half_rows), :]
            line = jnp.sum(jnp.where(on_diagonal, block, 0.0), axis=0, keepdims=True)
            for i in span:
                if i <= k:
                    mine = across[0:1] // half_rows == i - span[0]
                    diagonals[i, k] = jnp.sum(jnp.where(mine, line, 0.0), axis=1, keepdims=True)
    for e, pair in enumerate(pairs):
        row = jnp.where(lanes == e, diagonals[pair], row)
    tile_ref[...] = jnp.broadcast_to(row[None], tile_ref.shape)


def gram_call(residuals, block_pairs, new_owner, rows_count, device_count, pair_cap):
    order_n, held_slots, block_rows = residuals.shape[:3]
    half_rows = block_rows // 2
    return pl.pallas_call(
        functools.partial(gram_kernel, rows_count, pair_cap),
        out_shape=(
            pltpu.VMEM((device_count, 1, LANES), jnp.float32),
            pltpu.SMEM((rows_count * pair_cap + 1,), jnp.int32),
        ),
        in_specs=[pl.BlockSpec(memory_space=pltpu.HBM)] * 3,
        out_specs=(pl.BlockSpec(memory_space=pltpu.VMEM), pl.BlockSpec(memory_space=pltpu.SMEM)),
        scratch_shapes=[
            pltpu.VMEM(residuals.shape, residuals.dtype),
            pltpu.VMEM((order_n * half_rows, TILE * half_rows), jnp.float32),
            pltpu.VMEM(((order_n - TILE) * half_rows,) * 2, jnp.float32),
            pltpu.SMEM(new_owner.shape, jnp.int32),
            pltpu.SMEM(block_pairs.shape, jnp.int32),
            pltpu.SMEM((rows_count + 1,), jnp.int32),
            pltpu.SemaphoreType.DMA((held_slots // GRAM_SLOTS,)),
            pltpu.SemaphoreType.DMA((2,)),
        ],
        compiler_params=pltpu.CompilerParams(vmem_limit_bytes=24 * MIB),
        name="gram",
    )(new_owner, block_pairs, residuals)


def solve_rows(total, order_n):
    entry = {}
    for e, (i, k) in enumerate(pair_list(order_n)):
        entry[i, k] = jnp.broadcast_to(total[0:1, e:e + 1], (SUBLANES, LANES))
    vector = [jnp.ones((SUBLANES, LANES), jnp.float32)] * order_n
    for step in range(order_n):
        for i in range(step + 1, order_n):
            factor = entry[step, i] / entry[step, step]
            for k in range(i, order_n):
                entry[i, k] = entry[i, k] - factor * entry[step, k]
            vector[i] = vector[i] - factor * vector[step]
    solved = [None] * order_n
    for step in reversed(range(order_n)):
        inner = vector[step]
        for k in range(step + 1, order_n):
            inner = inner - entry[step, k] * solved[k]
        solved[step] = inner / entry[step, step]
    whole = functools.reduce(jnp.add, solved)
    return [x / whole for x in solved]


def fetch_copies(step, pair_cap, table_ref, densities_ref, residuals_ref, density_ref, residual_ref, sems):
    def copies(place):
        slot = table_ref[step * pair_cap + place]
        return (
            pltpu.make_async_copy(densities_ref.at[:, slot], density_ref.at[:, place], sems.at[0, place]),
            pltpu.make_async_copy(residuals_ref.at[:, slot], residual_ref.at[:, place], sems.at[1, place]),
        )

    return copies


def row_groups(ref):
    return [pl.ds(start, 2 * SUBLANES) for start in range(0, ref.shape[-2], 2 * SUBLANES)]


def moved(density_ref, residual_ref, index):
    return density_ref[index].astype(jnp.float32) + mix_weight * residual_ref[index].astype(jnp.float32)


def prepare_kernel(step, pair_cap, table_ref, densities_ref, residuals_ref, moved_ref, density_ref, residual_ref, sems):
    copies = fetch_copies(step, pair_cap, table_ref, densities_ref, residuals_ref, density_ref, residual_ref, sems)
    for place in range(pair_cap):
        for copy in copies(place):
            copy.start()
    for place in range(pair_cap):
        for copy in copies(place):
            copy.wait()
        for rows in row_groups(moved_ref):
            for i in range(moved_ref.shape[0]):
                moved_ref[i, place, rows, :] = moved(density_ref, residual_ref, (i, place, rows, slice(None)))


def prepare_call(step, pair_cap, table, densities, residuals):
    shape = (densities.shape[0], pair_cap) + densities.shape[2:]
    hbm = pl.BlockSpec(memory_space=pltpu.HBM)
    return pl.pallas_call(
        functools.partial(prepare_kernel, step, pair_cap),
        out_shape=pltpu.VMEM(shape, jnp.float32),
        in_specs=[pl.BlockSpec(memory_space=pltpu.SMEM), hbm, hbm],
        out_specs=pl.BlockSpec(memory_space=pltpu.VMEM),
        scratch_shapes=[
            pltpu.VMEM(shape, densities.dtype),
            pltpu.VMEM(shape, residuals.dtype),
            pltpu.SemaphoreType.DMA((2, pair_cap)),
        ],
        compiler_params=pltpu.CompilerParams(vmem_limit_bytes=12 * MIB),
        name="prepare",
    )(pltpu.with_memory_space_constraint(table, pltpu.SMEM), densities, residuals)


def first_kernel(tiles_ref, moved_ref, mixed_ref, coef_ref):
    order_n = moved_ref.shape[0]
    total = tiles_ref[0]
    for device in range(1, tiles_ref.shape[0]):
        total = total + tiles_ref[device]
    coefs = solve_rows(total, order_n)
    rows = lax.broadcasted_iota(jnp.int32, (SUBLANES, LANES), 0)
    stacked = jnp.zeros((SUBLANES, LANES), jnp.float32)
    for i in range(order_n):
        stacked = jnp.where(rows == i, coefs[i], stacked)
    coef_ref[...] = stacked
    coefs = [jnp.concatenate([c, c], axis=0) for c in coefs]
    for place in range(mixed_ref.shape[0]):
        for rows in row_groups(mixed_ref):
            running = None
            for i, coef in enumerate(coefs):
                term = coef * moved_ref[i, place, rows, :]
                running = term if running is None else running + term
            mixed_ref[place, rows, :] = running.astype(mixed_ref.dtype)


def first_call(tiles, moved_blocks):
    vmem = pl.BlockSpec(memory_space=pltpu.VMEM)
    keep = functools.partial(pltpu.with_memory_space_constraint, memory_space=pltpu.VMEM)
    return pl.pallas_call(
        first_kernel,
        out_shape=(
            pltpu.VMEM(moved_blocks.shape[1:], jnp.bfloat16),
            pltpu.VMEM((SUBLANES, LANES), jnp.float32),
        ),
        in_specs=[vmem] * 2,
        out_specs=(vmem, vmem),
        compiler_params=pltpu.CompilerParams(vmem_limit_bytes=8 * MIB),
        name="blend_first",
    )(keep(tiles), keep(moved_blocks))


def blend_kernel(step, pair_cap, table_ref, coef_ref, densities_ref, residuals_ref,
                 mixed_ref, density_ref, residual_ref, sems):
    order_n = densities_ref.shape[0]
    copies = fetch_copies(step, pair_cap, table_ref, densities_ref, residuals_ref, density_ref, residual_ref, sems)
    for place in range(pair_cap):
        for copy in copies(place):
            copy.start()
    coefs = [jnp.broadcast_to(coef_ref[i:i + 1, :], (2 * SUBLANES, LANES)) for i in range(order_n)]
    for place in range(pair_cap):
        for copy in copies(place):
            copy.wait()
        for rows in row_groups(mixed_ref):
            running = None
            for i, coef in enumerate(coefs):
                term = coef * moved(density_ref, residual_ref, (i, place, rows, slice(None)))
                running = term if running is None else running + term
            mixed_ref[place, rows, :] = running.astype(mixed_ref.dtype)


def blend_call(step, pair_cap, table, coef, densities, residuals):
    order_n = densities.shape[0]
    block = densities.shape[2:]
    vmem = pl.BlockSpec(memory_space=pltpu.VMEM)
    hbm = pl.BlockSpec(memory_space=pltpu.HBM)
    return pl.pallas_call(
        functools.partial(blend_kernel, step, pair_cap),
        out_shape=pltpu.VMEM((pair_cap,) + block, jnp.bfloat16),
        in_specs=[pl.BlockSpec(memory_space=pltpu.SMEM), vmem, hbm, hbm],
        out_specs=vmem,
        scratch_shapes=[
            pltpu.VMEM((order_n, pair_cap) + block, densities.dtype),
            pltpu.VMEM((order_n, pair_cap) + block, residuals.dtype),
            pltpu.SemaphoreType.DMA((2, pair_cap)),
        ],
        compiler_params=pltpu.CompilerParams(vmem_limit_bytes=8 * MIB),
    )(
        pltpu.with_memory_space_constraint(table, pltpu.SMEM),
        pltpu.with_memory_space_constraint(coef, pltpu.VMEM),
        densities,
        residuals,
    )


def place_kernel(steps, count_ref, offset_ref, *rest):
    arrived = rest[:len(steps)]
    owned_ref, sem = rest[-2:]

    def each(act):
        for n, step in enumerate(steps):
            count, offset = count_ref[step], offset_ref[step]
            size = arrived[n].shape[0]
            while size:
                before = count - lax.rem(count, 2 * size)

                @pl.when(lax.rem(count, 2 * size) >= size)
                def _():
                    act(pltpu.make_async_copy(
                        arrived[n].at[pl.ds(before, size)],
                        owned_ref.at[pl.ds(offset + before, size)],
                        sem.at[n, size.bit_length() - 1],
                    ))

                size //= 2

    each(lambda copy: copy.start())
    each(lambda copy: copy.wait())


def place_call(steps, counts, offsets, arrived, owned):
    pair_cap = arrived[0].shape[0]
    smem = pl.BlockSpec(memory_space=pltpu.SMEM)
    hbm = pl.BlockSpec(memory_space=pltpu.HBM)
    held = [pltpu.with_memory_space_constraint(x, pltpu.VMEM) for x in arrived]
    begun = [] if owned is None else [pltpu.with_memory_space_constraint(owned, pltpu.HBM)]
    return pl.pallas_call(
        functools.partial(place_kernel, steps),
        out_shape=pltpu.HBM((OWNED,) + arrived[0].shape[1:], arrived[0].dtype),
        in_specs=[smem, smem] + [pl.BlockSpec(memory_space=pltpu.VMEM)] * len(held) + [hbm] * len(begun),
        out_specs=hbm,
        scratch_shapes=[pltpu.SemaphoreType.DMA((len(held), pair_cap.bit_length()))],
        input_output_aliases={2 + len(held): 0} if begun else {},
        compiler_params=pltpu.CompilerParams(vmem_limit_bytes=4 * MIB),
        name="place",
    )(
        pltpu.with_memory_space_constraint(counts, pltpu.SMEM),
        pltpu.with_memory_space_constraint(offsets, pltpu.SMEM),
        *held,
        *begun,
    )


def step_order(rows_count):
    half = rows_count // 2
    far = [*range(half, rows_count)]
    near = [*range(half // 2, half), *range(1, half // 2)]
    return far[:half // 2] + near + far[half // 2:] + [0]


def on_device(densities, residuals, block_pairs, new_owner):
    rows_count = lax.axis_size("rows")
    cols_count = lax.axis_size("cols")
    order_n = densities.shape[0]
    densities = pltpu.with_memory_space_constraint(densities, pltpu.HBM)
    residuals = pltpu.with_memory_space_constraint(residuals, pltpu.HBM)
    pair_cap = 2 * OWNED // rows_count
    my_row, my_col = lax.axis_index("rows"), lax.axis_index("cols")
    order = step_order(rows_count)
    block_pairs = pltpu.with_memory_space_constraint(block_pairs, pltpu.HBM)
    new_owner = pltpu.with_memory_space_constraint(new_owner, pltpu.HBM)
    tiles, table = gram_call(
        residuals, block_pairs, new_owner, rows_count, rows_count * cols_count, pair_cap
    )
    tiles = lax.all_to_all(tiles, ("rows", "cols"), split_axis=0, concat_axis=0, tiled=True)
    moved_blocks = prepare_call(order[0], pair_cap, table, densities, residuals)

    arrived = [None] * rows_count
    coef = None
    for step in order:
        if coef is None:
            mixed, coef = first_call(tiles, moved_blocks)
        else:
            mixed = blend_call(step, pair_cap, table, coef, densities, residuals)
        if step:
            pairs = [(row, int(partner(row, step, rows_count))) for row in range(rows_count)]
            mixed = lax.ppermute(mixed, "rows", pairs)
        arrived[step] = mixed

    by_row = tiles.reshape(rows_count, cols_count, LANES)
    by_row = lax.dynamic_index_in_dim(by_row, my_col, 1, keepdims=False)
    by_row = lax.dynamic_index_in_dim(by_row, COUNT_LANE + my_row, 1, keepdims=False)
    row_ids = jnp.arange(rows_count, dtype=jnp.int32)
    from_row = row_ids ^ my_row if rows_count & (rows_count - 1) == 0 else (
        row_ids * -1 + my_row + rows_count) % rows_count
    counts = jnp.sum(jnp.where(from_row[:, None] == row_ids[None, :], by_row[None, :], 0.0), axis=1)
    offsets = jnp.sum(jnp.where(from_row[:, None] > row_ids[None, :], by_row[None, :], 0.0), axis=1)
    counts, offsets = counts.astype(jnp.int32), offsets.astype(jnp.int32)
    last = order[-2]
    early = [step for step in order if step != last]
    owned_blocks = place_call(early, counts, offsets, [arrived[step] for step in early], None)
    owned_blocks = place_call([last], counts, offsets, [arrived[last]], owned_blocks)
    return (owned_blocks, coef[:order_n, 0])


def solution(mesh):
    return jax.shard_map(
        on_device,
        mesh=mesh,
        in_specs=(
            P(None, ("rows", "cols"), None, None),
            P(None, ("rows", "cols"), None, None),
            P(None, ("rows", "cols")),
            P(("rows", "cols")),
        ),
        out_specs=(P(("rows", "cols"), None, None), P()),
        check_vma=False,
    )
```

```python
import functools

import jax
import jax.numpy as jnp
from jax import lax
from jax.experimental import pallas as pl
from jax.experimental.pallas import tpu as pltpu
from jax.sharding import PartitionSpec as P


OWNED = 32
LANES = 128
SUBLANES = 8
TILE = 4
GRAM_SLOTS = 16
COUNT_LANE = 64
MIB = 1024 * 1024

mix_weight = 0.3


def pair_list(order_n):
    return [(i, k) for i in range(order_n) for k in range(i, order_n)]


def partner(index, step, count):
    return index ^ step if count & (count - 1) == 0 else lax.rem(index + step, count)


def pattern_of(owner, index, count):
    return owner ^ index if count & (count - 1) == 0 else lax.rem(owner + count - index, count)


def gram_kernel(rows_count, pair_cap, owner_hbm, pairs_hbm, residuals_ref, tile_ref, table_ref,
                held_ref, low_ref, high_ref, owner_ref, pairs_ref, count_ref, sems, index_sems):
    order_n, held_slots = residuals_ref.shape[:2]
    pairs = pair_list(order_n)
    chunks = held_slots // GRAM_SLOTS

    def chunk_copy(chunk):
        span = pl.ds(chunk * GRAM_SLOTS, GRAM_SLOTS)
        return pltpu.make_async_copy(residuals_ref.at[:, span], held_ref.at[:, span], sems.at[chunk])

    index_copies = (
        pltpu.make_async_copy(owner_hbm, owner_ref, index_sems.at[0]),
        pltpu.make_async_copy(pairs_hbm, pairs_ref, index_sems.at[1]),
    )
    for copy in index_copies:
        copy.start()
    for chunk in range(chunks):
        chunk_copy(chunk).start()
    my_row = lax.axis_index("rows")
    sent_count = rows_count * pair_cap

    def clear(place, carry):
        table_ref[place] = 0
        return carry

    def route(slot):
        owner = owner_ref[slot]
        alive = owner >= 0
        bucket = jnp.where(alive, owner, rows_count)
        rank = count_ref[bucket]
        count_ref[bucket] = rank + 1
        place = pattern_of(owner, my_row, rows_count) * pair_cap + rank
        table_ref[jnp.where(alive, place, sent_count)] = slot

    for row in range(rows_count + 1):
        count_ref[row] = 0
    for ref in (low_ref, high_ref):
        ref[...] = jnp.zeros_like(ref)
    lax.fori_loop(0, sent_count, clear, 0, unroll=8)
    for copy in index_copies:
        copy.wait()

    block_rows = residuals_ref.shape[2]
    half_rows = block_rows // 2

    def weight_of(slot):
        alive = owner_ref[slot] >= 0
        diagonal = pairs_ref[0, slot] == pairs_ref[1, slot]
        return jnp.where(alive, jnp.where(diagonal, 1.0, 2.0), 0.0).astype(jnp.float32)

    def matrix_slots(slots):
        plain = [
            jnp.concatenate(
                [held_ref[i, slot, pl.ds(start, half_rows), :] for slot in slots for start in (0, half_rows)],
                axis=1,
            )
            for i in range(order_n)
        ]
        weight = jnp.concatenate(
            [jnp.full((half_rows, 2 * LANES), weight_of(slot), jnp.float32).astype(jnp.bfloat16) for slot in slots],
            axis=1,
        )
        scaled = [x * weight for x in plain]
        for ref, span in ((low_ref, range(TILE)), (high_ref, range(TILE, order_n))):
            ref[...] += lax.dot_general(
                jnp.concatenate(scaled[span[0]:], axis=0),
                jnp.concatenate([plain[i] for i in span], axis=0),
                (((1,), (1,)), ((), ())),
                preferred_element_type=jnp.float32,
            )

    def chunk_step(chunk, carry):
        chunk_copy(chunk).wait()
        slots = [chunk * GRAM_SLOTS + i for i in range(GRAM_SLOTS)]
        for slot in slots:
            route(slot)
        matrix_slots(slots)
        return carry

    lax.fori_loop(0, chunks, chunk_step, 0)

    lanes = lax.broadcasted_iota(jnp.int32, (1, LANES), 1)
    row = jnp.zeros((1, LANES), jnp.float32)
    for owner in range(rows_count):
        row = jnp.where(lanes == COUNT_LANE + owner, count_ref[owner].astype(jnp.float32), row)
    diagonals = {}
    for ref, span in ((low_ref, range(TILE)), (high_ref, range(TILE, order_n))):
        width = ref.shape[1]
        across = lax.broadcasted_iota(jnp.int32, (half_rows, width), 1)
        down = lax.broadcasted_iota(jnp.int32, (half_rows, width), 0)
        on_diagonal = across % half_rows == down
        for k in range(span[0], order_n):
            block = ref[pl.ds((k - span[0]) * half_rows, half_rows), :]
            line = jnp.sum(jnp.where(on_diagonal, block, 0.0), axis=0, keepdims=True)
            for i in span:
                if i <= k:
                    mine = across[0:1] // half_rows == i - span[0]
                    diagonals[i, k] = jnp.sum(jnp.where(mine, line, 0.0), axis=1, keepdims=True)
    for e, pair in enumerate(pairs):
        row = jnp.where(lanes == e, diagonals[pair], row)
    tile_ref[...] = jnp.broadcast_to(row[None], tile_ref.shape)


def gram_call(residuals, block_pairs, new_owner, rows_count, device_count, pair_cap):
    order_n, held_slots, block_rows = residuals.shape[:3]
    half_rows = block_rows // 2
    return pl.pallas_call(
        functools.partial(gram_kernel, rows_count, pair_cap),
        out_shape=(
            jax.ShapeDtypeStruct((device_count, 1, LANES), jnp.float32),
            pltpu.SMEM((rows_count * pair_cap + 1,), jnp.int32),
        ),
        in_specs=[pl.BlockSpec(memory_space=pltpu.HBM)] * 3,
        out_specs=(pl.BlockSpec(memory_space=pltpu.VMEM), pl.BlockSpec(memory_space=pltpu.SMEM)),
        scratch_shapes=[
            pltpu.VMEM(residuals.shape, residuals.dtype),
            pltpu.VMEM((order_n * half_rows, TILE * half_rows), jnp.float32),
            pltpu.VMEM(((order_n - TILE) * half_rows,) * 2, jnp.float32),
            pltpu.SMEM(new_owner.shape, jnp.int32),
            pltpu.SMEM(block_pairs.shape, jnp.int32),
            pltpu.SMEM((rows_count + 1,), jnp.int32),
            pltpu.SemaphoreType.DMA((held_slots // GRAM_SLOTS,)),
            pltpu.SemaphoreType.DMA((2,)),
        ],
        compiler_params=pltpu.CompilerParams(vmem_limit_bytes=20 * MIB),
        name="gram",
    )(new_owner, block_pairs, residuals)


def solve_rows(total, order_n):
    entry = {}
    for e, (i, k) in enumerate(pair_list(order_n)):
        entry[i, k] = jnp.broadcast_to(total[0:1, e:e + 1], (SUBLANES, LANES))
    vector = [jnp.ones((SUBLANES, LANES), jnp.float32)] * order_n
    for step in range(order_n):
        for i in range(step + 1, order_n):
            factor = entry[step, i] / entry[step, step]
            for k in range(i, order_n):
                entry[i, k] = entry[i, k] - factor * entry[step, k]
            vector[i] = vector[i] - factor * vector[step]
    solved = [None] * order_n
    for step in reversed(range(order_n)):
        inner = vector[step]
        for k in range(step + 1, order_n):
            inner = inner - entry[step, k] * solved[k]
        solved[step] = inner / entry[step, step]
    whole = functools.reduce(jnp.add, solved)
    return [x / whole for x in solved]


def fetch_copies(step, pair_cap, table_ref, densities_ref, residuals_ref, density_ref, residual_ref, sems):
    def copies(place):
        slot = table_ref[step * pair_cap + place]
        return (
            pltpu.make_async_copy(densities_ref.at[:, slot], density_ref.at[:, place], sems.at[0, place]),
            pltpu.make_async_copy(residuals_ref.at[:, slot], residual_ref.at[:, place], sems.at[1, place]),
        )

    return copies


def row_groups(ref):
    return [pl.ds(start, 2 * SUBLANES) for start in range(0, ref.shape[-2], 2 * SUBLANES)]


def moved(density_ref, residual_ref, index):
    return density_ref[index].astype(jnp.float32) + mix_weight * residual_ref[index].astype(jnp.float32)


def prepare_kernel(step, pair_cap, table_ref, densities_ref, residuals_ref, kept_ref, moved_ref, density_ref, residual_ref, sems):
    def keep(place, carry):
        kept_ref[place] = table_ref[place]
        return carry

    lax.fori_loop(0, table_ref.shape[0] - 1, keep, 0, unroll=8)
    copies = fetch_copies(step, pair_cap, table_ref, densities_ref, residuals_ref, density_ref, residual_ref, sems)
    for place in range(pair_cap):
        for copy in copies(place):
            copy.start()
    for place in range(pair_cap):
        for copy in copies(place):
            copy.wait()
        for rows in row_groups(moved_ref):
            for i in range(moved_ref.shape[0]):
                moved_ref[i, place, rows, :] = moved(density_ref, residual_ref, (i, place, rows, slice(None)))


def prepare_call(step, pair_cap, table, densities, residuals):
    shape = (densities.shape[0], pair_cap) + densities.shape[2:]
    hbm = pl.BlockSpec(memory_space=pltpu.HBM)
    return pl.pallas_call(
        functools.partial(prepare_kernel, step, pair_cap),
        out_shape=(pltpu.SMEM(table.shape, table.dtype), pltpu.VMEM(shape, jnp.float32)),
        in_specs=[pl.BlockSpec(memory_space=pltpu.SMEM), hbm, hbm],
        out_specs=(pl.BlockSpec(memory_space=pltpu.SMEM), pl.BlockSpec(memory_space=pltpu.VMEM)),
        scratch_shapes=[
            pltpu.VMEM(shape, densities.dtype),
            pltpu.VMEM(shape, residuals.dtype),
            pltpu.SemaphoreType.DMA((2, pair_cap)),
        ],
        compiler_params=pltpu.CompilerParams(vmem_limit_bytes=6 * MIB),
        name="prepare",
    )(pltpu.with_memory_space_constraint(table, pltpu.SMEM), densities, residuals)


def solve_tiles(tiles_ref, order_n):
    total = tiles_ref[0]
    for device in range(1, tiles_ref.shape[0]):
        total = total + tiles_ref[device]
    return solve_rows(total, order_n)


def first_kernel(tiles_ref, moved_ref, mixed_ref):
    coefs = [jnp.concatenate([c, c], axis=0) for c in solve_tiles(tiles_ref, moved_ref.shape[0])]
    for place in range(mixed_ref.shape[0]):
        for rows in row_groups(mixed_ref):
            running = None
            for i, coef in enumerate(coefs):
                term = coef * moved_ref[i, place, rows, :]
                running = term if running is None else running + term
            mixed_ref[place, rows, :] = running.astype(mixed_ref.dtype)


def coef_kernel(rows_count, cols_count, tiles_ref, coef_ref, list_ref, arrive_ref, offset_ref):
    rows = lax.broadcasted_iota(jnp.int32, (SUBLANES, LANES), 0)
    stacked = jnp.zeros((SUBLANES, LANES), jnp.float32)
    for i, coef in enumerate(solve_tiles(tiles_ref, list_ref.shape[0])):
        stacked = jnp.where(rows == i, coef, stacked)
        list_ref[i] = coef[0, 0]
    coef_ref[...] = stacked
    my_row, my_col = lax.axis_index("rows"), lax.axis_index("cols")
    mine = lax.broadcasted_iota(jnp.int32, (1, LANES), 1) == COUNT_LANE + my_row
    offset = 0
    for row in range(rows_count):
        count = jnp.sum(jnp.where(mine, tiles_ref[row * cols_count + my_col], 0.0)).astype(jnp.int32)
        step = pattern_of(my_row, row, rows_count)
        arrive_ref[step] = count
        offset_ref[step] = offset
        offset = offset + count


def coef_call(tiles, order_n, rows_count, cols_count):
    vmem = pl.BlockSpec(memory_space=pltpu.VMEM)
    smem = pl.BlockSpec(memory_space=pltpu.SMEM)
    table = pltpu.SMEM((rows_count,), jnp.int32)
    return pl.pallas_call(
        functools.partial(coef_kernel, rows_count, cols_count),
        out_shape=(
            pltpu.VMEM((SUBLANES, LANES), jnp.float32),
            jax.ShapeDtypeStruct((order_n,), jnp.float32),
            table,
            table,
        ),
        in_specs=[vmem],
        out_specs=(vmem, smem, smem, smem),
        compiler_params=pltpu.CompilerParams(vmem_limit_bytes=6 * MIB),
        name="coefs",
    )(pltpu.with_memory_space_constraint(tiles, pltpu.VMEM))


def held_call(kernel, out, *held):
    vmem = pl.BlockSpec(memory_space=pltpu.VMEM)
    return pl.pallas_call(
        kernel,
        out_shape=out,
        in_specs=[vmem] * len(held),
        out_specs=vmem,
        compiler_params=pltpu.CompilerParams(vmem_limit_bytes=6 * MIB),
    )(*[pltpu.with_memory_space_constraint(x, pltpu.VMEM) for x in held])


def blend_kernel(step, pair_cap, table_ref, coef_ref, densities_ref, residuals_ref,
                 mixed_ref, density_ref, residual_ref, sems):
    order_n = densities_ref.shape[0]
    copies = fetch_copies(step, pair_cap, table_ref, densities_ref, residuals_ref, density_ref, residual_ref, sems)
    for place in range(pair_cap):
        for copy in copies(place):
            copy.start()
    coefs = [jnp.broadcast_to(coef_ref[i:i + 1, :], (2 * SUBLANES, LANES)) for i in range(order_n)]
    for place in range(pair_cap):
        for copy in copies(place):
            copy.wait()
        for rows in row_groups(mixed_ref):
            running = None
            for i, coef in enumerate(coefs):
                term = coef * moved(density_ref, residual_ref, (i, place, rows, slice(None)))
                running = term if running is None else running + term
            mixed_ref[place, rows, :] = running.astype(mixed_ref.dtype)


def blend_call(step, pair_cap, table, coef, densities, residuals):
    order_n = densities.shape[0]
    block = densities.shape[2:]
    vmem = pl.BlockSpec(memory_space=pltpu.VMEM)
    hbm = pl.BlockSpec(memory_space=pltpu.HBM)
    return pl.pallas_call(
        functools.partial(blend_kernel, step, pair_cap),
        out_shape=pltpu.VMEM((pair_cap,) + block, jnp.bfloat16),
        in_specs=[pl.BlockSpec(memory_space=pltpu.SMEM), vmem, hbm, hbm],
        out_specs=vmem,
        scratch_shapes=[
            pltpu.VMEM((order_n, pair_cap) + block, densities.dtype),
            pltpu.VMEM((order_n, pair_cap) + block, residuals.dtype),
            pltpu.SemaphoreType.DMA((2, pair_cap)),
        ],
        compiler_params=pltpu.CompilerParams(vmem_limit_bytes=6 * MIB),
    )(
        pltpu.with_memory_space_constraint(table, pltpu.SMEM),
        pltpu.with_memory_space_constraint(coef, pltpu.VMEM),
        densities,
        residuals,
    )


def place_kernel(steps, count_ref, offset_ref, *rest):
    arrived = rest[:len(steps)]
    owned_ref, sem = rest[-2:]

    def each(act):
        for n, step in enumerate(steps):
            count, offset = count_ref[step], offset_ref[step]
            size = arrived[n].shape[0]
            while size:
                before = count - lax.rem(count, 2 * size)

                @pl.when(lax.rem(count, 2 * size) >= size)
                def _():
                    act(pltpu.make_async_copy(
                        arrived[n].at[pl.ds(before, size)],
                        owned_ref.at[pl.ds(offset + before, size)],
                        sem.at[n, size.bit_length() - 1],
                    ))

                size //= 2

    each(lambda copy: copy.start())
    each(lambda copy: copy.wait())


def place_call(steps, counts, offsets, arrived, owned):
    pair_cap = arrived[0].shape[0]
    smem = pl.BlockSpec(memory_space=pltpu.SMEM)
    hbm = pl.BlockSpec(memory_space=pltpu.HBM)
    held = [pltpu.with_memory_space_constraint(x, pltpu.VMEM) for x in arrived]
    begun = [] if owned is None else [pltpu.with_memory_space_constraint(owned, pltpu.HBM)]
    return pl.pallas_call(
        functools.partial(place_kernel, steps),
        out_shape=pltpu.HBM((OWNED,) + arrived[0].shape[1:], arrived[0].dtype),
        in_specs=[smem, smem] + [pl.BlockSpec(memory_space=pltpu.VMEM)] * len(held) + [hbm] * len(begun),
        out_specs=hbm,
        scratch_shapes=[pltpu.SemaphoreType.DMA((len(held), pair_cap.bit_length()))],
        input_output_aliases={2 + len(held): 0} if begun else {},
        compiler_params=pltpu.CompilerParams(vmem_limit_bytes=4 * MIB),
        name="place",
    )(
        pltpu.with_memory_space_constraint(counts, pltpu.SMEM),
        pltpu.with_memory_space_constraint(offsets, pltpu.SMEM),
        *held,
        *begun,
    )


def step_order(rows_count):
    half = rows_count // 2
    far = [*range(half, rows_count, 2), *range(half + 1, rows_count, 2)]
    near = [*range(half // 2, half), *range(1, half // 2)]
    return far[:half // 2] + near + far[half // 2:] + [0]


def placing_stages(order):
    count = len(order)
    late = [order[count // 2 - 1], *order[-1 - count // 4:-2]]
    last = order[-2]
    return [[step for step in order if step not in late and step != last], late, [last]]


def on_device(densities, residuals, block_pairs, new_owner):
    rows_count = lax.axis_size("rows")
    cols_count = lax.axis_size("cols")
    order_n = densities.shape[0]
    densities = pltpu.with_memory_space_constraint(densities, pltpu.HBM)
    residuals = pltpu.with_memory_space_constraint(residuals, pltpu.HBM)
    pair_cap = 2 * OWNED // rows_count
    order = step_order(rows_count)
    block_pairs = pltpu.with_memory_space_constraint(block_pairs, pltpu.HBM)
    new_owner = pltpu.with_memory_space_constraint(new_owner, pltpu.HBM)
    tiles, table = gram_call(
        residuals, block_pairs, new_owner, rows_count, rows_count * cols_count, pair_cap
    )
    tiles = lax.all_to_all(tiles, ("rows", "cols"), split_axis=0, concat_axis=0, tiled=True)
    table, moved_blocks = prepare_call(order[0], pair_cap, table, densities, residuals)

    arrived = [None] * rows_count
    coef = None
    for step in order:
        if step != order[0] and coef is None:
            coef, coefficients, counts, offsets = coef_call(tiles, order_n, rows_count, cols_count)
        if coef is None:
            out = pltpu.VMEM(moved_blocks.shape[1:], jnp.bfloat16)
            mixed = held_call(first_kernel, out, tiles, moved_blocks)
        else:
            mixed = blend_call(step, pair_cap, table, coef, densities, residuals)
        if step:
            pairs = [(row, int(partner(row, step, rows_count))) for row in range(rows_count)]
            mixed = lax.ppermute(mixed, "rows", pairs)
        arrived[step] = mixed

    owned_blocks = None
    for steps in placing_stages(order):
        owned_blocks = place_call(steps, counts, offsets, [arrived[step] for step in steps], owned_blocks)
    return (owned_blocks, coefficients)


def solution(mesh):
    return jax.shard_map(
        on_device,
        mesh=mesh,
        in_specs=(
            P(None, ("rows", "cols"), None, None),
            P(None, ("rows", "cols"), None, None),
            P(None, ("rows", "cols")),
            P(("rows", "cols")),
        ),
        out_specs=(P(("rows", "cols"), None, None), P()),
        check_vma=False,
    )
```
